16 devices in a mesh: dp: 2 (over y, z), cp: 8 (over x, core).
Axes of the slice: x: 4, y: 2, z: 1, core: 2. Of those that a mesh axis runs over, the one named last changes fastest.
The devices are a block of a 4x4x8 slice.
Arguments:
- x: bfloat16 [4096, 3072], P(('dp', 'cp')), parts along dimension 0
- seg: int32 [4096], P(('dp', 'cp')), parts along dimension 0
- wq: bfloat16 [3072, 3072], replicated
- wk: bfloat16 [3072, 1024], replicated
- wv: bfloat16 [3072, 1024], replicated
- wo: bfloat16 [3072, 3072], replicated
Outputs:
- output: bfloat16 [4096, 3072], P(('dp', 'cp')), parts along dimension 0
There are 2 independent parts. The reference program is written for one: setup_inputs(seed, part) draws one part's arguments, and reference() takes and returns one part's arrays. A program takes and returns all parts, laid end to end along the dimension named above; an argument that names none is the same for every part.
All inputs are finite; a program needn't handle non-finite values.
Results may differ from the reference program's by a relative error of at most 0.00626007.
Values are sent between devices in bfloat16 or wider.
A program may use at most 768 MiB of HBM per device.

```python
import jax
import jax.numpy as jnp
from jax import lax
import numpy as np

CP = 8
L = 256
D = 3072
HQ = 24
HKV = 8
DH = 128

S = CP * L
HALF = L // 2
G = HQ // HKV
QB = min(128, HALF)


def row_positions():
    rows = []
    for d in range(CP):
        rows.append(np.arange(d * HALF, (d + 1) * HALF))
        rows.append(np.arange((2 * CP - 1 - d) * HALF, (2 * CP - d) * HALF))
    return np.concatenate(rows).astype(np.int32)


def setup_inputs(seed: int = 0, part: int = 0) -> dict:
    key = jax.random.key(seed)
    kshared, kpart = jax.random.split(key)
    kp = jax.random.fold_in(kpart, part)
    kx, _, _ = jax.random.split(kp, 3)
    kd = jax.random.fold_in(kp, 7)
    ku, kc, kl = jax.random.split(kd, 3)
    kq, kk, kv, ko = jax.random.split(kshared, 4)
    x = jax.random.normal(kx, (S, D), jnp.float32).astype(jnp.bfloat16)
    token_pos = jnp.arange(S, dtype=jnp.int32)
    long_end = jax.random.randint(kl, (), 3 * S // 10, 7 * S // 10, jnp.int32)
    coin_flip = jax.random.randint(kc, (2 * CP,), 0, 2, jnp.int32)
    break_bar = jnp.repeat(jnp.where(coin_flip == 0, jnp.int32(1 << 22), jnp.int32((1 << 24) // L)), HALF)
    draw_bits = (jax.random.bits(ku, (S,), jnp.uint32) >> 8).astype(jnp.int32)
    breaks = (draw_bits < break_bar) & (token_pos > long_end)
    seg_orig = 7 + jnp.cumsum(breaks.astype(jnp.int32))
    seg = seg_orig[jnp.asarray(row_positions())].astype(jnp.int32)
    wq = (jax.random.normal(kq, (D, HQ * DH), jnp.float32) * (2.0 * D ** -0.5)).astype(jnp.bfloat16)
    wk = (jax.random.normal(kk, (D, HKV * DH), jnp.float32) * D ** -0.5).astype(jnp.bfloat16)
    wv = (jax.random.normal(kv, (D, HKV * DH), jnp.float32) * D ** -0.5).astype(jnp.bfloat16)
    wo = (jax.random.normal(ko, (HQ * DH, D), jnp.float32) * (HQ * DH) ** -0.5).astype(jnp.bfloat16)
    return {"x": x, "seg": seg, "wq": wq, "wk": wk, "wv": wv, "wo": wo}


def reference(x, seg, wq, wk, wv, wo):
    pos = jnp.asarray(row_positions())
    q = jnp.dot(x, wq, preferred_element_type=jnp.float32).astype(jnp.bfloat16)
    k = jnp.dot(x, wk, preferred_element_type=jnp.float32).astype(jnp.bfloat16)
    v = jnp.dot(x, wv, preferred_element_type=jnp.float32).astype(jnp.bfloat16)
    kf = k.astype(jnp.float32).reshape(S, HKV, DH)
    vf = v.astype(jnp.float32).reshape(S, HKV, DH)
    qb = q.reshape(S // QB, QB, HKV, G, DH)
    pb = pos.reshape(S // QB, QB)
    sb = seg.reshape(S // QB, QB)

    def block(args):
        qi, pi, si = args
        s = jnp.einsum("qhgd,khd->hgqk", qi.astype(jnp.float32), kf) * DH ** -0.5
        allowed = (si[:, None] == seg[None, :]) & (pos[None, :] <= pi[:, None])
        s = jnp.where(allowed, s, -jnp.inf)
        p = jax.nn.softmax(s, axis=-1)
        o = jnp.einsum("hgqk,khd->qhgd", p, vf)
        return o.astype(jnp.bfloat16)

    o = lax.map(block, (qb, pb, sb)).reshape(S, HQ * DH)
    return jnp.dot(o, wo, preferred_element_type=jnp.float32).astype(jnp.bfloat16)
```

```python
import functools
import math

import jax
import jax.numpy as jnp
from jax import lax
from jax.experimental import pallas as pl
from jax.experimental.pallas import tpu as pltpu
from jax.sharding import PartitionSpec as P

DH = 128
F32 = jnp.float32
BF16 = jnp.bfloat16
NEG = float("-inf")
SCALE = math.log2(math.e) * DH ** -0.5


def kernel(
    n, heads, groups,
    x_hbm, seg_hbm, wq_hbm, wk_hbm, wv_hbm, wo_hbm, y_hbm,
    x_buf, wkv, wq, wo, kv, q_buf, seg_all, bias, o_buf, o_sib, y_acc, y_out,
    x_sem, xs_send, xs_recv, seg_sem, sg_send, sg_recv, wkv_sem, wq_sem, wo_sem,
    own_send, near_recv, fwd_send, far_recv, os_send, os_recv, y_sem,
):
    chips = n // 2
    piece = x_hbm.shape[1]
    me = lax.axis_index("cp")
    c, h = lax.div(me, 2), lax.rem(me, 2)
    other = 1 - h
    right_chip, left_chip = lax.rem(c + 1, chips), lax.rem(c + chips - 1, chips)
    right, left, sibling = 2 * right_chip + h, 2 * left_chip + h, 2 * c + other
    qcols = heads * groups * DH

    def remote(src, dst, send, recv, dev):
        return pltpu.make_async_remote_copy(
            src_ref=src, dst_ref=dst, send_sem=send, recv_sem=recv,
            device_id={"cp": dev}, device_id_type=pl.DeviceIdType.MESH)

    x_own = pltpu.make_async_copy(x_hbm, x_buf.at[:, h], x_sem)
    x_own.start()
    seg_own = pltpu.make_async_copy(seg_hbm, seg_all.at[me], seg_sem)
    seg_own.start()

    def wkv_copies(g):
        col = pl.multiple_of((h * heads + g) * DH, DH)
        return [
            pltpu.make_async_copy(w.at[:, pl.ds(col, DH)], wkv.at[g, :, pl.ds(i * DH, DH)], wkv_sem.at[g, i])
            for i, w in enumerate((wk_hbm, wv_hbm))
        ]

    def wq_copy(t):
        col = pl.multiple_of(h * qcols + t * 2 * DH, 2 * DH)
        return pltpu.make_async_copy(wq_hbm.at[:, pl.ds(col, 2 * DH)], wq.at[t], wq_sem.at[t])

    gw = groups * DH

    def wo_copies(g):
        res = []
        for i, core in enumerate((h, other)):
            row = pl.multiple_of(core * qcols + g * gw, DH)
            res.append(pltpu.make_async_copy(wo_hbm.at[pl.ds(row, gw)], wo.at[g, pl.ds(i * gw, gw)], wo_sem.at[g, i]))
        return res

    for g in range(heads):
        for cp in wkv_copies(g):
            cp.start()

    barrier = pltpu.get_barrier_semaphore()
    for d in range(1, n):
        pl.semaphore_signal(barrier, inc=1, device_id={"cp": lax.rem(me + d, n)}, device_id_type=pl.DeviceIdType.MESH)
    pl.semaphore_wait(barrier, n - 1)

    x_send = remote(x_hbm, x_buf.at[:, h], xs_send, xs_recv, sibling)
    x_send.start()
    n_q = wq.shape[0]
    for t in range(n_q):
        wq_copy(t).start()
    for g in range(heads):
        for cp in wo_copies(g):
            cp.start()
    seg_own.wait()
    seg_sends = []
    for d in range(1, n):
        cp = remote(seg_all.at[me], seg_all.at[me], sg_send.at[d - 1], sg_recv.at[d - 1], lax.rem(me + d, n))
        cp.start()
        seg_sends.append(cp)

    def own(g, r, to_right):
        s = 0 if to_right else 1
        ref = kv.at[g, :, c, r]
        return remote(ref, ref, own_send.at[s, g, r], near_recv.at[s, g, r], right if to_right else left)

    def near_wait(g, r, from_left):
        s = 0 if from_left else 1
        ref = kv.at[g, :, left_chip if from_left else right_chip, r]
        remote(ref, ref, own_send.at[s, g, r], near_recv.at[s, g, r], right if from_left else left).wait_recv()

    def fwd(g, to_right):
        s = 0 if to_right else 1
        ref = kv.at[g, :, left_chip if to_right else right_chip, 0 if to_right else 1]
        return remote(ref, ref, fwd_send.at[s, g], far_recv.at[s, g], right if to_right else left)

    far_chip = lax.rem(c + chips // 2, chips)

    def far_wait(g, s):
        ref = kv.at[g, :, far_chip, s]
        remote(ref, ref, fwd_send.at[s, g], far_recv.at[s, g], right if s == 0 else left).wait_recv()

    def forward(g):
        for to_right in (True, False):
            near_wait(g, 0 if to_right else 1, to_right)
            fwd(g, to_right).start()

    def send_own_rows(g, r):
        own(g, r, True).start()
        own(g, r, False).start()

    def send_first(g):
        own(g, 0, True).start()
        own(g, 1, False).start()

    def send_second(g):
        own(g, 1, True).start()
        own(g, 0, False).start()

    def wait_head(g):
        near_wait(g, 1, True)
        near_wait(g, 0, False)
        far_wait(g, 0)
        far_wait(g, 1)

    def proj_rows(g, r):
        rows = x_buf[:, r].reshape(2 * piece, x_buf.shape[-1])
        res = jnp.dot(rows, wkv[g], preferred_element_type=F32).astype(BF16)
        kv[g, :, c, r] = res.reshape(2, piece, 2 * DH)

    def proj_all(g):
        rows = x_buf[...].reshape(4 * piece, x_buf.shape[-1])
        res = jnp.dot(rows, wkv[g], preferred_element_type=F32).astype(BF16)
        kv[g, :, c] = res.reshape(2, 2, piece, 2 * DH)

    def proj_q(t):
        rows = x_buf[...].reshape(4 * piece, x_buf.shape[-1])
        res = jnp.dot(rows, wq[t], preferred_element_type=F32).astype(BF16)
        q_buf[2 * t] = res[:, :DH]
        q_buf[2 * t + 1] = res[:, DH:]

    def make_bias():
        for fs in range(2):
            for r in range(2):
                dev = 2 * c + r
                base = (dev if fs == 0 else 2 * n - 1 - dev) * piece
                sq = jnp.broadcast_to(seg_all[dev, pl.ds(fs, 1)], (piece, piece)).T
                pq = base + lax.broadcasted_iota(jnp.int32, (piece, piece), 0)
                for kfs in range(fs + 1):
                    for kd in range(n):
                        kbase = (kd if kfs == 0 else 2 * n - 1 - kd) * piece
                        sk = seg_all[kd, pl.ds(kfs, 1)]
                        pk = kbase + lax.broadcasted_iota(jnp.int32, (piece, piece), 1)
                        ok = (sq == sk) & (pk <= pq)
                        col = (kfs * n + kd) * piece
                        bias[fs, pl.ds(r * piece, piece), pl.ds(col, piece)] = jnp.where(ok, 0.0, NEG).astype(F32)

    def attend(g, j, fs):
        rows = 2 * piece
        nk = (fs + 1) * n * piece
        q = q_buf[g * groups + j, pl.ds(fs * rows, rows)]
        k = kv[g, pl.ds(0, fs + 1), :, :, :, pl.ds(0, DH)].reshape(nk, DH)
        v = kv[g, pl.ds(0, fs + 1), :, :, :, pl.ds(DH, DH)].reshape(nk, DH)
        s = lax.dot_general(q, k, (((1,), (1,)), ((), ())), preferred_element_type=F32)
        s = s + bias[fs, :, pl.ds(0, nk)]
        m = jnp.max(s, axis=-1, keepdims=True)
        p = jnp.exp2(s * SCALE - m * SCALE)
        l = jnp.sum(p, axis=-1, keepdims=True)
        o = jnp.dot(p.astype(BF16), v, preferred_element_type=F32) / l
        o_buf[g, fs, :, :, pl.ds(j * DH, DH)] = o.astype(BF16).reshape(2, piece, DH)

    def attention(g):
        for j in range(groups):
            attend(g, j, 0)
            attend(g, j, 1)

    def o_send(g):
        return remote(o_buf.at[g, :, other], o_sib.at[g], os_send.at[g], os_recv.at[g], sibling)

    nt = 4
    tile = wo.shape[-1] // nt

    def y_copy(t):
        col = pl.ds(pl.multiple_of(t * tile, tile), tile)
        return pltpu.make_async_copy(y_out.at[:, col], y_hbm.at[:, col], y_sem.at[t])

    def out_proj(g):
        for cp in wo_copies(g):
            cp.wait()
        o_send(g).wait_recv()
        mine = o_buf[g, :, h].reshape(2 * piece, gw)
        theirs = o_sib[g].reshape(2 * piece, gw)
        lhs = jnp.concatenate([mine, theirs], axis=-1)

        def body(t, carry):
            col = pl.ds(pl.multiple_of(t * tile, tile), tile)
            acc = jnp.dot(lhs, wo[g, :, col], preferred_element_type=F32)
            if g > 0:
                acc = acc + y_acc[:, col]
            if g < heads - 1:
                y_acc[:, col] = acc
            else:
                y_out[:, col] = acc.astype(BF16)
                y_copy(t).start()
            return carry

        lax.fori_loop(0, nt, body, 0)

    x_own.wait()
    for cp in wkv_copies(0):
        cp.wait()
    proj_rows(0, h)
    send_own_rows(0, h)
    remote(x_hbm, x_buf.at[:, other], xs_send, xs_recv, sibling).wait_recv()
    proj_rows(0, other)
    send_own_rows(0, other)
    for g in range(1, heads):
        for cp in wkv_copies(g):
            cp.wait()
        proj_all(g)
        if g == 1:
            send_first(1)
    half_q = n_q // 2
    for t in range(half_q):
        wq_copy(t).wait()
        proj_q(t)
    forward(0)
    send_second(1)
    for t in range(half_q, n_q):
        wq_copy(t).wait()
        proj_q(t)
    for d in range(1, n):
        src = lax.rem(me + n - d, n)
        remote(seg_all.at[src], seg_all.at[src], sg_send.at[d - 1], sg_recv.at[d - 1], src).wait_recv()
    make_bias()
    send_first(2)
    forward(1)
    send_second(2)
    wait_head(0)
    attention(0)
    o_send(0).start()
    send_first(3)
    forward(2)
    send_second(3)
    wait_head(1)
    attention(1)
    o_send(1).start()
    out_proj(0)
    forward(3)
    wait_head(2)
    attention(2)
    o_send(2).start()
    out_proj(1)
    wait_head(3)
    attention(3)
    o_send(3).start()
    out_proj(2)
    out_proj(3)

    x_send.wait_send()
    for cp in seg_sends:
        cp.wait_send()
    for g in range(heads):
        for r in range(2):
            own(g, r, True).wait_send()
            own(g, r, False).wait_send()
        fwd(g, True).wait_send()
        fwd(g, False).wait_send()
        o_send(g).wait_send()
    for t in range(nt):
        y_copy(t).wait()


def solution(mesh):
    n = mesh.shape["cp"]
    chips = n // 2

    def local(x, seg, wq, wk, wv, wo):
        lq, d = x.shape
        piece = lq // 2
        kvh = wk.shape[1] // DH
        groups = wq.shape[1] // wk.shape[1]
        heads = kvh // 2
        qh = heads * groups
        dma = pltpu.SemaphoreType.DMA
        return pl.pallas_call(
            functools.partial(kernel, n, heads, groups),
            out_shape=jax.ShapeDtypeStruct((lq, wo.shape[1]), BF16),
            in_specs=[pl.BlockSpec(memory_space=pl.ANY)] * 6,
            out_specs=pl.BlockSpec(memory_space=pl.ANY),
            scratch_shapes=[
                pltpu.VMEM((2, 2, piece, d), BF16),
                pltpu.VMEM((heads, d, 2 * DH), BF16),
                pltpu.VMEM((qh // 2, d, 2 * DH), BF16),
                pltpu.VMEM((heads, 2 * groups * DH, wo.shape[1]), BF16),
                pltpu.VMEM((heads, 2, chips, 2, piece, 2 * DH), BF16),
                pltpu.VMEM((qh, 2 * lq, DH), BF16),
                pltpu.VMEM((n, 2, piece), jnp.int32),
                pltpu.VMEM((2, lq, n * lq), F32),
                pltpu.VMEM((heads, 2, 2, piece, groups * DH), BF16),
                pltpu.VMEM((heads, 2, piece, groups * DH), BF16),
                pltpu.VMEM((lq, wo.shape[1]), F32),
                pltpu.VMEM((lq, wo.shape[1]), BF16),
                dma, dma, dma, dma, dma((n - 1,)), dma((n - 1,)),
                dma((heads, 2)), dma((qh // 2,)), dma((heads, 2)),
                dma((2, heads, 2)), dma((2, heads, 2)), dma((2, heads)), dma((2, heads)),
                dma((heads,)), dma((heads,)), dma((4,)),
            ],
            compiler_params=pltpu.CompilerParams(
                collective_id=0, has_side_effects=True, vmem_limit_bytes=67043328),
            name="fused_attention",
        )(x.reshape(2, piece, d), seg.reshape(2, piece), wq, wk, wv, wo)

    rows = P(("dp", "cp"), None)
    return jax.shard_map(local, mesh=mesh, in_specs=(rows, P(("dp", "cp")), P(), P(), P(), P()), out_specs=rows, check_vma=False)
```

```python
import functools
import math

import jax
import jax.numpy as jnp
from jax import lax
from jax.experimental import pallas as pl
from jax.experimental.pallas import tpu as pltpu
from jax.sharding import PartitionSpec as P

DH = 128
F32 = jnp.float32
BF16 = jnp.bfloat16
NEG = float("-inf")
SCALE = math.log2(math.e) * DH ** -0.5


def kernel(
    n, heads, groups,
    x_hbm, seg_hbm, wq_hbm, wk_hbm, wv_hbm, wo_hbm, y_out,
    x_buf, wkv, wq, wo, kv, q_buf, seg_all, bias, s_buf, m_buf, l_buf, c_buf, a_buf, o_buf, o_sib, y_acc,
    x_sem, xs_send, xs_recv, seg_sem, sg_send, sg_recv, wkv_sem, wq_sem, wo_sem,
    own_send, near_recv, fwd_send, far_recv, os_send, os_recv,
):
    chips = n // 2
    piece = x_hbm.shape[1]
    rows = 2 * piece
    dim = x_hbm.shape[2]
    me = lax.axis_index("cp")
    c, h = lax.div(me, 2), lax.rem(me, 2)
    other = 1 - h
    right_chip, left_chip = lax.rem(c + 1, chips), lax.rem(c + chips - 1, chips)
    far_chip = lax.rem(c + chips // 2, chips)
    right, left, sibling = 2 * right_chip + h, 2 * left_chip + h, 2 * c + other
    qcols = heads * groups * DH
    gw = groups * DH
    ph = jax.named_scope

    def remote(src, dst, send, recv, dev):
        return pltpu.make_async_remote_copy(
            src_ref=src, dst_ref=dst, send_sem=send, recv_sem=recv,
            device_id={"cp": dev}, device_id_type=pl.DeviceIdType.MESH)

    def wkv_copies(t):
        res = []
        for i in range(2):
            col = pl.multiple_of((h * heads + 2 * t + i) * DH, DH)
            for j, w in enumerate((wk_hbm, wv_hbm)):
                dst = wkv.at[t, :, pl.ds((2 * i + j) * DH, DH)]
                res.append(pltpu.make_async_copy(w.at[:, pl.ds(col, DH)], dst, wkv_sem.at[t, i, j]))
        return res

    qt = wq.shape[-1]
    n_q = wq.shape[0]

    def wq_copy(t):
        col = pl.multiple_of(h * qcols + t * qt, qt)
        return pltpu.make_async_copy(wq_hbm.at[:, pl.ds(col, qt)], wq.at[t], wq_sem.at[t])

    def wo_copies(g):
        res = []
        for i, core in enumerate((h, other)):
            row = pl.multiple_of(core * qcols + g * gw, DH)
            res.append(pltpu.make_async_copy(wo_hbm.at[pl.ds(row, gw)], wo.at[g, pl.ds(i * gw, gw)], wo_sem.at[g, i]))
        return res

    def own(g, r, to_right):
        s = 0 if to_right else 1
        ref = kv.at[g, :, c, r]
        return remote(ref, ref, own_send.at[s, g, r], near_recv.at[s, g, r], right if to_right else left)

    def near_wait(g, r, from_left):
        s = 0 if from_left else 1
        ref = kv.at[g, :, left_chip if from_left else right_chip, r]
        remote(ref, ref, own_send.at[s, g, r], near_recv.at[s, g, r], right if from_left else left).wait_recv()

    def fwd(g, to_right):
        s = 0 if to_right else 1
        ref = kv.at[g, :, left_chip if to_right else right_chip, 0 if to_right else 1]
        return remote(ref, ref, fwd_send.at[s, g], far_recv.at[s, g], right if to_right else left)

    def far_wait(g):
        for s in range(2):
            ref = kv.at[g, :, far_chip, s]
            remote(ref, ref, fwd_send.at[s, g], far_recv.at[s, g], right if s == 0 else left).wait_recv()

    def forward(g):
        for to_right in (True, False):
            near_wait(g, 0 if to_right else 1, to_right)
            fwd(g, to_right).start()

    def send_rows(g, r):
        own(g, r, True).start()
        own(g, r, False).start()

    def send_first(g):
        own(g, 0, True).start()
        own(g, 1, False).start()

    def send_second(g):
        own(g, 1, True).start()
        own(g, 0, False).start()

    def proj_kv(t, r):
        src = x_buf[:, r].reshape(rows, dim)
        res = jnp.dot(src, wkv[t], preferred_element_type=F32)
        for i in range(2):
            kv[2 * t + i, :, c, r, 0] = res[:, 2 * i * DH:(2 * i + 1) * DH].astype(BF16).reshape(2, piece, DH)
            for f in range(2):
                v = res[f * piece:(f + 1) * piece, (2 * i + 1) * DH:2 * (i + 1) * DH]
                kv[2 * t + i, f, c, r, 1] = v.T.astype(BF16)

    def proj_q(t, r):
        src = x_buf[:, r].reshape(rows, dim)
        res = jnp.dot(src, wq[t], preferred_element_type=F32).astype(BF16)
        per = qt // DH
        for i in range(per):
            q_buf[per * t + i, :, r] = res[:, i * DH:(i + 1) * DH].reshape(2, piece, DH)

    def dyn(chip):
        return (chip > c).astype(jnp.int32)

    near_static = [(0, 0, c), (1, 1, c), (1, 0, c), (1, 0, left_chip), (1, 0, right_chip)]
    near_dyn = [(dyn(left_chip), dyn(left_chip), left_chip), (dyn(right_chip), dyn(right_chip), right_chip)]
    far_blocks = [(1, 0, far_chip), (dyn(far_chip), dyn(far_chip), far_chip)]
    blocks = near_static + near_dyn + far_blocks

    def first_row(half, dev):
        return jnp.where(half == 0, dev, 2 * n - 1 - dev) * piece

    def make_bias():
        for b, (qs, ks, kc) in enumerate(blocks):
            for r in range(2):
                dev = 2 * c + r
                sq = seg_all[dev, pl.ds(qs, 1)]
                pq = first_row(qs, dev) + lax.broadcasted_iota(jnp.int32, (piece, piece), 1)
                for kr in range(2):
                    kd = 2 * kc + kr
                    sk = jnp.broadcast_to(seg_all[kd, pl.ds(ks, 1)], (piece, piece)).T
                    pk = first_row(ks, kd) + lax.broadcasted_iota(jnp.int32, (piece, piece), 0)
                    ok = (sq == sk) & (pk <= pq)
                    bias[b, pl.ds(kr * piece, piece), pl.ds(r * piece, piece)] = jnp.where(ok, 0.0, NEG).astype(F32)

    def scores(g, j, b):
        qs, ks, kc = blocks[b]
        q = q_buf[g * groups + j, qs].reshape(rows, DH)
        k = kv[g, ks, kc, :, 0].reshape(rows, DH)
        s = lax.dot_general(k, q, (((1,), (1,)), ((), ())), preferred_element_type=F32)
        return s + bias[b]

    def top(s):
        return jnp.max(s, axis=0, keepdims=True)

    def values(g, b):
        return jnp.concatenate([kv[g, blocks[b][1], blocks[b][2], r, 1] for r in range(2)], axis=1)

    def region(fn):
        pl.when(me >= 0)(fn)

    def attend(g, bs, start):
        st = g % 2 * groups

        def score_all():
            for j in range(groups):
                m = [None, None] if start else [m_buf[st + j, 0], m_buf[st + j, 1]]
                for i, b in enumerate(bs):
                    s = scores(g, j, b)
                    s_buf[j, i] = s
                    t = top(s)
                    half = blocks[b][0]
                    for f in range(2):
                        if isinstance(half, int):
                            v = t if half == f else None
                        else:
                            v = jnp.where(half == f, t, NEG)
                        if v is not None:
                            m[f] = v if m[f] is None else jnp.maximum(m[f], v)
                for f in range(2):
                    if not start:
                        c_buf[j, f] = jnp.exp2(m_buf[st + j, f] * SCALE - m[f] * SCALE)
                    m_buf[st + j, f] = m[f]

        def weigh_all():
            for j in range(groups):
                l, a = [0.0, 0.0], [0.0, 0.0]
                if not start:
                    l = [l_buf[st + j, f] * c_buf[j, f] for f in range(2)]
                    a = [a_buf[st + j, f] * c_buf[j, f] for f in range(2)]
                late = []
                for i, b in enumerate(bs):
                    half = blocks[b][0]
                    p = jnp.exp2(s_buf[j, i] * SCALE - m_buf[st + j, half] * SCALE)
                    lb = jnp.sum(p, axis=0, keepdims=True)
                    ab = jnp.dot(values(g, b), p.astype(BF16), preferred_element_type=F32)
                    if isinstance(half, int):
                        l[half], a[half] = l[half] + lb, a[half] + ab
                    else:
                        late.append((half, lb, ab))
                if start:
                    for f in range(2):
                        l_buf[st + j, f], a_buf[st + j, f] = l[f], a[f]
                    for half, lb, ab in late:
                        l_buf[st + j, half] = l_buf[st + j, half] + lb
                        a_buf[st + j, half] = a_buf[st + j, half] + ab
                else:
                    for f in range(2):
                        for half, lb, ab in late:
                            l[f] = l[f] + jnp.where(half == f, lb, 0.0)
                            a[f] = a[f] + jnp.where(half == f, ab, 0.0)
                        o = a[f] * (1.0 / l[f])
                        o_buf[g, f, :, :, pl.ds(j * DH, DH)] = o.T.astype(BF16).reshape(2, piece, DH)

        region(score_all)
        region(weigh_all)

    near_ids = list(range(len(near_static) + len(near_dyn)))
    far_ids = [len(near_ids), len(near_ids) + 1]

    def near(g):
        attend(g, near_ids, True)

    def far(g):
        attend(g, far_ids, False)

    def o_send(g):
        return remote(o_buf.at[g, :, other], o_sib.at[g], os_send.at[g], os_recv.at[g], sibling)

    nt = 3
    tile = wo.shape[-1] // nt

    def mine(g):
        return o_buf[g, :, h].reshape(rows, gw)

    def theirs(g):
        return o_sib[g].reshape(rows, gw)

    def project(lhs, rhs, first, last):
        for t in range(nt):
            col = pl.ds(t * tile, tile)
            acc = jnp.dot(lhs, rhs(col), preferred_element_type=F32)
            if not first:
                acc = acc + y_acc[:, col]
            if last:
                y_out[:, col] = acc.astype(BF16)
            else:
                y_acc[:, col] = acc

    def wo_wait(g):
        for cp in wo_copies(g):
            cp.wait()

    def out_proj(gs):
        lhs = []
        for g in gs:
            wo_wait(g)
            o_send(g).wait_recv()
            lhs += [mine(g), theirs(g)]
        project(jnp.concatenate(lhs, axis=-1),
                lambda col: wo[pl.ds(gs[0], len(gs)), :, col].reshape(len(gs) * 2 * gw, tile), gs[0] == 0, False)

    x_own = pltpu.make_async_copy(x_hbm, x_buf.at[:, h], x_sem)
    x_own.start()
    seg_own = pltpu.make_async_copy(seg_hbm, seg_all.at[me], seg_sem)
    seg_own.start()
    n_kv = wkv.shape[0]
    barrier = pltpu.get_barrier_semaphore()
    for d in range(1, n):
        pl.semaphore_signal(barrier, inc=1, device_id={"cp": lax.rem(me + d, n)}, device_id_type=pl.DeviceIdType.MESH)
    for t in range(n_kv):
        for cp in wkv_copies(t):
            cp.start()
    for t in range(n_q):
        wq_copy(t).start(priority=1)

    with ph("wait_x"):
        x_own.wait()
        for cp in wkv_copies(0):
            cp.wait()
        seg_own.wait()
    with ph("kv0a"):
        proj_kv(0, h)

    with ph("barrier"):
        pl.semaphore_wait(barrier, n - 1)
    x_send = remote(x_buf.at[:, h], x_buf.at[:, h], xs_send, xs_recv, sibling)
    x_send.start()
    send_rows(0, h)
    send_rows(1, h)
    seg_sends = []
    for d in range(1, n):
        cp = remote(seg_all.at[me], seg_all.at[me], sg_send.at[d - 1], sg_recv.at[d - 1], lax.rem(me + d, n))
        cp.start()
        seg_sends.append(cp)
    for g in range(heads):
        for cp in wo_copies(g):
            cp.start(priority=1)
    with ph("kv1a"):
        for cp in wkv_copies(1):
            cp.wait()
        proj_kv(1, h)
    with ph("qa"):
        for t in range(n_q - 1):
            wq_copy(t).wait()
            proj_q(t, h)
    with ph("wait_xs"):
        remote(x_buf.at[:, other], x_buf.at[:, other], xs_send, xs_recv, sibling).wait_recv()
    with ph("kv0b"):
        proj_kv(0, other)
    send_rows(0, other)
    send_rows(1, other)
    with ph("kv1b"):
        proj_kv(1, other)
    with ph("qb"):
        wq_copy(n_q - 1).wait()
        proj_q(n_q - 1, h)
        for t in range(n_q):
            proj_q(t, other)
    with ph("wait_seg"):
        for d in range(1, n):
            src = lax.rem(me + n - d, n)
            remote(seg_all.at[src], seg_all.at[src], sg_send.at[d - 1], sg_recv.at[d - 1], src).wait_recv()
    with ph("bias"):
        make_bias()

    def near_rest(g):
        near_wait(g, 1, True)
        near_wait(g, 0, False)

    with ph("fwd0"):
        forward(0)
    send_first(2)
    send_second(2)
    with ph("nwait0"):
        near_rest(0)
    with ph("near0"):
        near(0)
    with ph("fwd1"):
        forward(1)
    send_first(3)
    send_second(3)
    with ph("nwait1"):
        near_rest(1)
    with ph("near1"):
        near(1)
    with ph("fwait0"):
        far_wait(0)
    with ph("far0"):
        far(0)
    o_send(0).start()
    with ph("fwd2"):
        forward(2)
    with ph("nwait2"):
        near_rest(2)
    with ph("near2"):
        near(2)
    with ph("fwait1"):
        far_wait(1)
    with ph("far1"):
        far(1)
    o_send(1).start()
    with ph("out0"):
        out_proj((0,))
    with ph("fwd3"):
        forward(3)
    with ph("out1"):
        out_proj((1,))
    with ph("nwait3"):
        near_rest(3)
    with ph("near3"):
        near(3)
    with ph("fwait2"):
        far_wait(2)
    with ph("far2"):
        far(2)
    o_send(2).start()
    with ph("fwait3"):
        far_wait(3)
    with ph("far3"):
        far(3)
    o_send(3).start()
    with ph("out2"):
        out_proj((2,))
    wo_wait(3)
    with ph("out3a"):
        project(mine(3), lambda col: wo[3, pl.ds(0, gw), col], False, False)
    with ph("owait"):
        o_send(3).wait_recv()
    with ph("out3b"):
        project(theirs(3), lambda col: wo[3, pl.ds(gw, gw), col], False, True)

    with ph("drain"):
        x_send.wait_send()
        for cp in seg_sends:
            cp.wait_send()
        for g in range(heads):
            for r in range(2):
                own(g, r, True).wait_send()
                own(g, r, False).wait_send()
            fwd(g, True).wait_send()
            fwd(g, False).wait_send()
            o_send(g).wait_send()


def solution(mesh):
    n = mesh.shape["cp"]
    chips = n // 2

    def local(x, seg, wq, wk, wv, wo):
        lq, d = x.shape
        piece = lq // 2
        kvh = wk.shape[1] // DH
        groups = wq.shape[1] // wk.shape[1]
        heads = kvh // 2
        qh = heads * groups
        dma = pltpu.SemaphoreType.DMA
        return pl.pallas_call(
            functools.partial(kernel, n, heads, groups),
            out_shape=pltpu.VMEM((lq, wo.shape[1]), BF16),
            in_specs=[pl.BlockSpec(memory_space=pl.ANY)] * 6,
            out_specs=pl.BlockSpec(memory_space=pltpu.VMEM),
            scratch_shapes=[
                pltpu.VMEM((2, 2, piece, d), BF16),
                pltpu.VMEM((heads // 2, d, 4 * DH), BF16),
                pltpu.VMEM((qh // 4, d, 4 * DH), BF16),
                pltpu.VMEM((heads, 2 * groups * DH, wo.shape[1]), BF16),
                pltpu.VMEM((heads, 2, chips, 2, 2, piece, DH), BF16),
                pltpu.VMEM((qh, 2, 2, piece, DH), BF16),
                pltpu.VMEM((n, 2, piece), jnp.int32),
                pltpu.VMEM((9, lq, lq), F32),
                pltpu.VMEM((groups, 7, lq, lq), F32),
                pltpu.VMEM((2 * groups, 2, 1, lq), F32),
                pltpu.VMEM((2 * groups, 2, 1, lq), F32),
                pltpu.VMEM((groups, 2, 1, lq), F32),
                pltpu.VMEM((2 * groups, 2, DH, lq), F32),
                pltpu.VMEM((heads, 2, 2, piece, groups * DH), BF16),
                pltpu.VMEM((heads, 2, piece, groups * DH), BF16),
                pltpu.VMEM((lq, wo.shape[1]), F32),
                dma, dma, dma, dma, dma((n - 1,)), dma((n - 1,)),
                dma((heads // 2, 2, 2)), dma((qh // 4,)), dma((heads, 2)),
                dma((2, heads, 2)), dma((2, heads, 2)), dma((2, heads)), dma((2, heads)),
                dma((heads,)), dma((heads,)),
            ],
            compiler_params=pltpu.CompilerParams(
                collective_id=0, has_side_effects=True, vmem_limit_bytes=67043328 - (2 << 20)),
            name="fused_attention",
        )(x.reshape(2, piece, d), seg.reshape(2, piece), wq, wk, wv, wo)

    rows = P(("dp", "cp"), None)
    return jax.shard_map(local, mesh=mesh, in_specs=(rows, P(("dp", "cp")), P(), P(), P(), P()), out_specs=rows, check_vma=False)
```

```python
import functools
import math

import jax
import jax.numpy as jnp
from jax import lax
from jax.experimental import pallas as pl
from jax.experimental.pallas import tpu as pltpu
from jax.sharding import PartitionSpec as P

DH = 128
F32 = jnp.float32
BF16 = jnp.bfloat16
NEG = float("-inf")
SCALE = math.log2(math.e) * DH ** -0.5


def kernel(
    n, heads, groups,
    x_hbm, seg_hbm, wq_hbm, wk_hbm, wv_hbm, wo_hbm, y_out,
    x_buf, wkv, wq, wo, kv, q_buf, seg_all, bias, s_buf, m_buf, l_buf, c_buf, a_buf, o_buf, o_sib, y_acc,
    x_sem, xs_send, xs_recv, seg_sem, sg_send, sg_recv, wkv_sem, wq_sem, wo_sem,
    kv_send, near_recv, far_recv, os_send, os_recv,
):
    chips = n // 2
    parts = wkv_sem.shape[1]
    piece = x_hbm.shape[1]
    rows = 2 * piece
    dim = x_hbm.shape[2]
    me = lax.axis_index("cp")
    c, h = lax.div(me, 2), lax.rem(me, 2)
    other = 1 - h
    right_chip, left_chip = lax.rem(c + 1, chips), lax.rem(c + chips - 1, chips)
    far_chip = lax.rem(c + chips // 2, chips)
    right, left, sibling = 2 * right_chip + h, 2 * left_chip + h, 2 * c + other
    qcols = heads * groups * DH
    gw = groups * DH
    ph = jax.named_scope

    def remote(src, dst, send, recv, dev):
        return pltpu.make_async_remote_copy(
            src_ref=src, dst_ref=dst, send_sem=send, recv_sem=recv,
            device_id={"cp": dev}, device_id_type=pl.DeviceIdType.MESH)

    def wkv_part(g, part):
        return (pl.ds(part * dim // parts, dim // parts), pl.ds(g % 2 * 2 * DH, 2 * DH))

    def wkv_start(g):
        col = pl.multiple_of((h * heads + g) * DH, DH)
        for part in range(parts):
            rng, at = wkv_part(g, part)
            for j, w in enumerate((wk_hbm, wv_hbm)):
                dst = wkv.at[g // 2, rng, pl.ds(at.start + j * DH, DH)]
                pltpu.make_async_copy(w.at[rng, pl.ds(col, DH)], dst, wkv_sem.at[g, part]).start()

    def wkv_wait(g, part):
        ref = wkv.at[g // 2, *wkv_part(g, part)]
        pltpu.make_async_copy(ref, ref, wkv_sem.at[g, part]).wait()

    qt = wq.shape[-1]
    n_q = wq.shape[0]

    def wq_copy(t):
        col = pl.multiple_of(h * qcols + t * qt, qt)
        return pltpu.make_async_copy(wq_hbm.at[:, pl.ds(col, qt)], wq.at[t], wq_sem.at[t])

    def wo_copies(g):
        res = []
        for i, core in enumerate((h, other)):
            row = pl.multiple_of(core * qcols + g * gw, DH)
            res.append(pltpu.make_async_copy(wo_hbm.at[pl.ds(row, gw)], wo.at[g, pl.ds(i * gw, gw)], wo_sem.at[g]))
        return res

    seg_others = seg_all.at[pl.ds(0, n - 1)]

    def own(g, r, to_right):
        s = 0 if to_right else 1
        ref = kv.at[g, :, c, r]
        return remote(ref, ref, kv_send.at[g], near_recv.at[s, g, r], right if to_right else left)

    def near_wait(g, r, from_left):
        s = 0 if from_left else 1
        ref = kv.at[g, :, left_chip if from_left else right_chip, r]
        remote(ref, ref, kv_send.at[g], near_recv.at[s, g, r], right if from_left else left).wait_recv()

    def fwd(g, to_right):
        s = 0 if to_right else 1
        ref = kv.at[g, :, left_chip if to_right else right_chip, 0 if to_right else 1]
        return remote(ref, ref, kv_send.at[g], far_recv.at[s, g], right if to_right else left)

    def far_wait(g):
        for s in range(2):
            ref = kv.at[g, :, far_chip, s]
            remote(ref, ref, kv_send.at[g], far_recv.at[s, g], right if s == 0 else left).wait_recv()

    def forward(g):
        for to_right in (True, False):
            near_wait(g, 0 if to_right else 1, to_right)
            fwd(g, to_right).start()

    def send_rows(g, r):
        own(g, r, True).start()
        own(g, r, False).start()

    def send_first(g):
        own(g, 0, True).start()
        own(g, 1, False).start()

    def send_second(g):
        own(g, 1, True).start()
        own(g, 0, False).start()

    def keep_kv(g, r, k, v):
        kv[g, :, c, r, 0] = k.astype(BF16).reshape(2, piece, DH)
        for f in range(2):
            kv[g, f, c, r, 1] = v[f * piece:(f + 1) * piece].T.astype(BF16)

    def proj_head(g, r):
        res = 0.0
        for part in range(parts):
            wkv_wait(g, part)
            rng, at = wkv_part(g, part)
            src = x_buf[:, r, :, rng].reshape(rows, rng.size)
            res = res + jnp.dot(src, wkv[g // 2, rng, at], preferred_element_type=F32)
        keep_kv(g, r, res[:, :DH], res[:, DH:])

    def proj_kv(t, r):
        src = x_buf[:, r].reshape(rows, dim)
        res = jnp.dot(src, wkv[t], preferred_element_type=F32)
        for i in range(2):
            k = 2 * i * DH
            keep_kv(2 * t + i, r, res[:, k:k + DH], res[:, k + DH:k + 2 * DH])

    def proj_q(t, r):
        src = x_buf[:, r].reshape(rows, dim)
        res = jnp.dot(src, wq[t], preferred_element_type=F32).astype(BF16)
        per = qt // DH
        for i in range(per):
            q_buf[per * t + i, :, r] = res[:, i * DH:(i + 1) * DH].reshape(2, piece, DH)

    def dyn(chip):
        return (chip > c).astype(jnp.int32)

    near_static = [(0, 0, c), (1, 1, c), (1, 0, c), (1, 0, left_chip), (1, 0, right_chip)]
    near_dyn = [(dyn(left_chip), dyn(left_chip), left_chip), (dyn(right_chip), dyn(right_chip), right_chip)]
    far_blocks = [(1, 0, far_chip), (dyn(far_chip), dyn(far_chip), far_chip)]
    blocks = near_static + near_dyn + far_blocks

    def first_row(half, dev):
        return jnp.where(half == 0, dev, 2 * n - 1 - dev) * piece

    def make_bias():
        for b, (qs, ks, kc) in enumerate(blocks):
            for r in range(2):
                dev = 2 * c + r
                sq = seg_all[dev, pl.ds(qs, 1)]
                pq = first_row(qs, dev) + lax.broadcasted_iota(jnp.int32, (piece, piece), 1)
                for kr in range(2):
                    kd = 2 * kc + kr
                    sk = jnp.broadcast_to(seg_all[kd, pl.ds(ks, 1)], (piece, piece)).T
                    pk = first_row(ks, kd) + lax.broadcasted_iota(jnp.int32, (piece, piece), 0)
                    ok = (sq == sk) & (pk <= pq)
                    bias[b, pl.ds(kr * piece, piece), pl.ds(r * piece, piece)] = jnp.where(ok, 0.0, NEG).astype(F32)

    def scores(g, j, b):
        qs, ks, kc = blocks[b]
        q = q_buf[g * groups + j, qs].reshape(rows, DH)
        k = kv[g, ks, kc, :, 0].reshape(rows, DH)
        s = lax.dot_general(k, q, (((1,), (1,)), ((), ())), preferred_element_type=F32)
        return s + bias[b]

    def top(s):
        return jnp.max(s, axis=0, keepdims=True)

    def values(g, b):
        return jnp.concatenate([kv[g, blocks[b][1], blocks[b][2], r, 1] for r in range(2)], axis=1)

    def region(fn):
        pl.when(me >= 0)(fn)

    def attend(g, bs, first, last):
        def score_all():
            for j in range(groups):
                k = g * groups + j
                m = [None, None] if first else [m_buf[k, 0], m_buf[k, 1]]
                for i, b in enumerate(bs):
                    s = scores(g, j, b)
                    s_buf[j, i] = s
                    t = top(s)
                    half = blocks[b][0]
                    for f in range(2):
                        if isinstance(half, int):
                            v = t if half == f else None
                        else:
                            v = jnp.where(half == f, t, NEG)
                        if v is not None:
                            m[f] = v if m[f] is None else jnp.maximum(m[f], v)
                for f in range(2):
                    if not first:
                        c_buf[j, f] = jnp.exp2(m_buf[k, f] * SCALE - m[f] * SCALE)
                    m_buf[k, f] = m[f]

        def weigh_all():
            for j in range(groups):
                k = g * groups + j
                l, a = [0.0, 0.0], [0.0, 0.0]
                if not first:
                    l = [l_buf[k, f] * c_buf[j, f] for f in range(2)]
                    a = [a_buf[k, f] * c_buf[j, f] for f in range(2)]
                late = []
                for i, b in enumerate(bs):
                    half = blocks[b][0]
                    p = jnp.exp2(s_buf[j, i] * SCALE - m_buf[k, half] * SCALE)
                    lb = jnp.sum(p, axis=0, keepdims=True)
                    ab = jnp.dot(values(g, b), p.astype(BF16), preferred_element_type=F32)
                    if isinstance(half, int):
                        l[half], a[half] = l[half] + lb, a[half] + ab
                    else:
                        late.append((half, lb, ab))
                if last:
                    for f in range(2):
                        for half, lb, ab in late:
                            l[f] = l[f] + jnp.where(half == f, lb, 0.0)
                            a[f] = a[f] + jnp.where(half == f, ab, 0.0)
                        o = a[f] * (1.0 / l[f])
                        o_buf[g, f, :, :, pl.ds(j * DH, DH)] = o.T.astype(BF16).reshape(2, piece, DH)
                else:
                    for f in range(2):
                        l_buf[k, f], a_buf[k, f] = l[f], a[f]
                    for half, lb, ab in late:
                        l_buf[k, half] = l_buf[k, half] + lb
                        a_buf[k, half] = a_buf[k, half] + ab

        region(score_all)
        region(weigh_all)

    def here(g):
        attend(g, [0, 1, 2], True, False)

    def near(g):
        attend(g, [3, 4, 5, 6], False, False)

    def far(g):
        attend(g, [7, 8], False, True)

    def o_send(g):
        return remote(o_buf.at[g, :, other], o_sib.at[g], os_send, os_recv.at[g], sibling)

    nt = 3
    tile = wo.shape[-1] // nt

    def mine(g):
        return o_buf[g, :, h].reshape(rows, gw)

    def theirs(g):
        return o_sib[g].reshape(rows, gw)

    def project(lhs, rhs, first, last):
        for t in range(nt):
            col = pl.ds(t * tile, tile)
            acc = jnp.dot(lhs, rhs(col), preferred_element_type=F32)
            if not first:
                acc = acc + y_acc[:, col]
            if last:
                y_out[:, col] = acc.astype(BF16)
            else:
                y_acc[:, col] = acc

    def wo_wait(g):
        pltpu.make_async_copy(wo.at[g], wo.at[g], wo_sem.at[g]).wait()

    def out_proj(gs):
        lhs = []
        for g in gs:
            wo_wait(g)
            o_send(g).wait_recv()
            lhs += [mine(g), theirs(g)]
        project(jnp.concatenate(lhs, axis=-1),
                lambda col: wo[pl.ds(gs[0], len(gs)), :, col].reshape(len(gs) * 2 * gw, tile), gs[0] == 0, False)

    x_own = pltpu.make_async_copy(x_hbm, x_buf.at[:, h], x_sem)
    x_own.start()
    seg_own = pltpu.make_async_copy(seg_hbm, seg_all.at[me], seg_sem)
    seg_own.start()
    barrier = pltpu.get_barrier_semaphore()
    for d in range(1, n):
        pl.semaphore_signal(barrier, inc=1, device_id={"cp": lax.rem(me + d, n)}, device_id_type=pl.DeviceIdType.MESH)
    for g in range(heads):
        wkv_start(g)
    for t in range(n_q):
        wq_copy(t).start(priority=1)

    with ph("wait_x"):
        x_own.wait()
        seg_own.wait()
    with ph("kv0a"):
        proj_head(0, h)

    with ph("barrier"):
        pl.semaphore_wait(barrier, n - 1)
    x_send = remote(x_buf.at[:, h], x_buf.at[:, h], xs_send, xs_recv, sibling)
    x_send.start()
    send_rows(0, h)
    for d in range(1, n):
        remote(seg_all.at[me], seg_all.at[me], sg_send, sg_recv, lax.rem(me + d, n)).start()
    for g in range(heads):
        for cp in wo_copies(g):
            cp.start(priority=1)
    with ph("kv0c"):
        proj_head(1, h)
    send_rows(1, h)
    with ph("kv1a"):
        for g in range(2, heads):
            for part in range(parts):
                wkv_wait(g, part)
        proj_kv(1, h)
    with ph("qa"):
        for t in range(n_q - 1):
            wq_copy(t).wait()
            proj_q(t, h)
    with ph("wait_xs"):
        remote(x_buf.at[:, other], x_buf.at[:, other], xs_send, xs_recv, sibling).wait_recv()
    with ph("kv0b"):
        proj_kv(0, other)
    send_rows(0, other)
    send_rows(1, other)
    with ph("kv1b"):
        proj_kv(1, other)
    with ph("qb"):
        wq_copy(n_q - 1).wait()
        proj_q(n_q - 1, h)
        for t in range(n_q):
            proj_q(t, other)
    with ph("wait_seg"):
        remote(seg_others, seg_others, sg_send, sg_recv, sibling).wait_recv()
    with ph("bias"):
        make_bias()

    def near_rest(g):
        near_wait(g, 1, True)
        near_wait(g, 0, False)

    with ph("fwd0"):
        forward(0)
    send_first(2)
    send_second(2)
    with ph("here0"):
        here(0)
    with ph("nwait0"):
        near_rest(0)
    with ph("near0"):
        near(0)
    with ph("fwd1"):
        forward(1)
    send_first(3)
    with ph("here1"):
        here(1)
    with ph("nwait1"):
        near_rest(1)
    with ph("near1"):
        near(1)
    with ph("fwait0"):
        far_wait(0)
    with ph("far0"):
        far(0)
    o_send(0).start()
    with ph("here2"):
        here(2)
    with ph("fwd2"):
        forward(2)
    send_second(3)
    with ph("here3"):
        here(3)
    with ph("nwait2"):
        near_rest(2)
    with ph("near2"):
        near(2)
    with ph("fwait1"):
        far_wait(1)
    with ph("far1"):
        far(1)
    o_send(1).start()
    with ph("out0"):
        out_proj((0,))
    with ph("fwd3"):
        forward(3)
    with ph("out1"):
        out_proj((1,))
    with ph("fwait2"):
        far_wait(2)
    with ph("far2"):
        far(2)
    o_send(2).start()
    with ph("nwait3"):
        near_rest(3)
    with ph("near3"):
        near(3)
    with ph("out2"):
        out_proj((2,))
    with ph("fwait3"):
        far_wait(3)
    with ph("far3"):
        far(3)
    o_send(3).start()
    wo_wait(3)
    with ph("out3a"):
        project(mine(3), lambda col: wo[3, pl.ds(0, gw), col], False, False)
    with ph("owait"):
        o_send(3).wait_recv()
    with ph("out3b"):
        project(theirs(3), lambda col: wo[3, pl.ds(gw, gw), col], False, True)

    with ph("drain"):
        x_send.wait_send()
        remote(seg_others, seg_others, sg_send, sg_recv, sibling).wait_send()
        for g in range(heads):
            sent = kv.at[g, :, pl.ds(0, chips - 1)]
            remote(sent, sent, kv_send.at[g], near_recv.at[0, 0, 0], right).wait_send()
        remote(o_sib, o_sib, os_send, os_recv.at[0], sibling).wait_send()


def solution(mesh):
    n = mesh.shape["cp"]
    chips = n // 2

    def local(x, seg, wq, wk, wv, wo):
        lq, d = x.shape
        piece = lq // 2
        kvh = wk.shape[1] // DH
        groups = wq.shape[1] // wk.shape[1]
        heads = kvh // 2
        qh = heads * groups
        dma = pltpu.SemaphoreType.DMA
        return pl.pallas_call(
            functools.partial(kernel, n, heads, groups),
            out_shape=pltpu.VMEM((lq, wo.shape[1]), BF16),
            in_specs=[pl.BlockSpec(memory_space=pl.ANY)] * 6,
            out_specs=pl.BlockSpec(memory_space=pltpu.VMEM),
            scratch_shapes=[
                pltpu.VMEM((2, 2, piece, d), BF16),
                pltpu.VMEM((heads // 2, d, 4 * DH), BF16),
                pltpu.VMEM((qh // 4, d, 4 * DH), BF16),
                pltpu.VMEM((heads, 2 * groups * DH, wo.shape[1]), BF16),
                pltpu.VMEM((heads, 2, chips, 2, 2, piece, DH), BF16),
                pltpu.VMEM((qh, 2, 2, piece, DH), BF16),
                pltpu.VMEM((n, 2, piece), jnp.int32),
                pltpu.VMEM((9, lq, lq), F32),
                pltpu.VMEM((groups, 4, lq, lq), F32),
                pltpu.VMEM((qh, 2, 1, lq), F32),
                pltpu.VMEM((qh, 2, 1, lq), F32),
                pltpu.VMEM((groups, 2, 1, lq), F32),
                pltpu.VMEM((qh, 2, DH, lq), F32),
                pltpu.VMEM((heads, 2, 2, piece, groups * DH), BF16),
                pltpu.VMEM((heads, 2, piece, groups * DH), BF16),
                pltpu.VMEM((lq, wo.shape[1]), F32),
                dma, dma, dma, dma, dma, dma,
                dma((heads, 4)), dma((qh // 4,)), dma((heads,)),
                dma((heads,)), dma((2, heads, 2)), dma((2, heads)),
                dma, dma((heads,)),
            ],
            compiler_params=pltpu.CompilerParams(
                collective_id=0, has_side_effects=True, vmem_limit_bytes=67043328 - (2 << 20)),
            name="fused_attention",
        )(x.reshape(2, piece, d), seg.reshape(2, piece), wq, wk, wv, wo)

    rows = P(("dp", "cp"), None)
    return jax.shard_map(local, mesh=mesh, in_specs=(rows, P(("dp", "cp")), P(), P(), P(), P()), out_specs=rows, check_vma=False)
```

```python
import functools
import math

import jax
import jax.numpy as jnp
from jax import lax
from jax.experimental import pallas as pl
from jax.experimental.pallas import tpu as pltpu
from jax.sharding import PartitionSpec as P

DH = 128
F32 = jnp.float32
BF16 = jnp.bfloat16
NEG = float("-inf")
SCALE = math.log2(math.e) * DH ** -0.5


def kernel(
    n, heads, groups,
    x_hbm, seg_hbm, wq_hbm, wk_hbm, wv_hbm, wo_hbm, y_out,
    x_buf, wkv, wq, wo, kv, q_buf, seg_all, bias, s_buf, m_buf, l_buf, c_buf, a_buf, o_buf, o_sib, y_acc,
    x_sem, xs_send, xs_recv, seg_sem, sg_send, sg_recv, wkv_sem, wq_sem, wo_sem,
    kv_send, near_recv, far_recv, os_send, os_recv,
):
    chips = n // 2
    parts = wkv_sem.shape[1]
    piece = x_hbm.shape[1]
    rows = 2 * piece
    dim = x_hbm.shape[2]
    me = lax.axis_index("cp")
    c, h = lax.div(me, 2), lax.rem(me, 2)
    other = 1 - h
    right_chip, left_chip = lax.rem(c + 1, chips), lax.rem(c + chips - 1, chips)
    far_chip = lax.rem(c + chips // 2, chips)
    right, left, sibling = 2 * right_chip + h, 2 * left_chip + h, 2 * c + other
    qcols = heads * groups * DH
    gw = groups * DH
    ph = jax.named_scope

    def remote(src, dst, send, recv, dev):
        return pltpu.make_async_remote_copy(
            src_ref=src, dst_ref=dst, send_sem=send, recv_sem=recv,
            device_id={"cp": dev}, device_id_type=pl.DeviceIdType.MESH)

    def wkv_part(g, part):
        return (pl.ds(part * dim // parts, dim // parts), pl.ds(g % 2 * 2 * DH, 2 * DH))

    def wkv_start(g):
        col = pl.multiple_of((h * heads + g) * DH, DH)
        for part in range(parts):
            rng, at = wkv_part(g, part)
            for j, w in enumerate((wk_hbm, wv_hbm)):
                dst = wkv.at[g // 2, rng, pl.ds(at.start + j * DH, DH)]
                pltpu.make_async_copy(w.at[rng, pl.ds(col, DH)], dst, wkv_sem.at[g, part]).start()

    def wkv_wait(g, part):
        ref = wkv.at[g // 2, *wkv_part(g, part)]
        pltpu.make_async_copy(ref, ref, wkv_sem.at[g, part]).wait()

    qt = wq.shape[-1]
    n_q = wq.shape[0]

    def wq_copy(t):
        col = pl.multiple_of(h * qcols + t * qt, qt)
        return pltpu.make_async_copy(wq_hbm.at[:, pl.ds(col, qt)], wq.at[t], wq_sem.at[t])

    def wo_copies(g):
        res = []
        for i, core in enumerate((h, other)):
            row = pl.multiple_of(core * qcols + g * gw, DH)
            res.append(pltpu.make_async_copy(wo_hbm.at[pl.ds(row, gw)], wo.at[g, pl.ds(i * gw, gw)], wo_sem.at[g]))
        return res

    seg_others = seg_all.at[pl.ds(0, n - 1)]

    def own(g, r, to_right):
        s = 0 if to_right else 1
        ref = kv.at[g, :, c, r]
        return remote(ref, ref, kv_send.at[g], near_recv.at[s, g, r], right if to_right else left)

    def near_wait(g, r, from_left):
        s = 0 if from_left else 1
        ref = kv.at[g, :, left_chip if from_left else right_chip, r]
        remote(ref, ref, kv_send.at[g], near_recv.at[s, g, r], right if from_left else left).wait_recv()

    def halves(g):
        return ((g, slice(None)),) if g < heads - 1 else ((g, pl.ds(0, 1)), (heads, pl.ds(1, 1)))

    def fwd(g, to_right):
        s = 0 if to_right else 1
        refs = [(i, kv.at[g, f, left_chip if to_right else right_chip, s]) for i, f in halves(g)]
        return [remote(ref, ref, kv_send.at[g], far_recv.at[s, i], right if to_right else left) for i, ref in refs]

    def far_wait(g, half=0):
        i, f = halves(g)[half]
        for s in range(2):
            ref = kv.at[g, f, far_chip, s]
            remote(ref, ref, kv_send.at[g], far_recv.at[s, i], right if s == 0 else left).wait_recv()

    def forward(g):
        for to_right in (True, False):
            near_wait(g, 0 if to_right else 1, to_right)
            for cp in fwd(g, to_right):
                cp.start()

    def send_rows(g, r):
        own(g, r, True).start()
        own(g, r, False).start()

    def send_first(g):
        own(g, 0, True).start()
        own(g, 1, False).start()

    def send_second(g):
        own(g, 1, True).start()
        own(g, 0, False).start()

    def keep_kv(g, r, k, v):
        kv[g, :, c, r, 0] = k.astype(BF16).reshape(2, piece, DH)
        for f in range(2):
            kv[g, f, c, r, 1] = v[f * piece:(f + 1) * piece].T.astype(BF16)

    def proj_head(g, r):
        res = 0.0
        for part in range(parts):
            wkv_wait(g, part)
            rng, at = wkv_part(g, part)
            src = x_buf[:, r, :, rng].reshape(rows, rng.size)
            res = res + jnp.dot(src, wkv[g // 2, rng, at], preferred_element_type=F32)
        keep_kv(g, r, res[:, :DH], res[:, DH:])

    def proj_kv(t, r):
        src = x_buf[:, r].reshape(rows, dim)
        res = jnp.dot(src, wkv[t], preferred_element_type=F32)
        for i in range(2):
            k = 2 * i * DH
            keep_kv(2 * t + i, r, res[:, k:k + DH], res[:, k + DH:k + 2 * DH])

    def proj_q(t, r):
        src = x_buf[:, r].reshape(rows, dim)
        res = jnp.dot(src, wq[t], preferred_element_type=F32).astype(BF16)
        per = qt // DH
        for i in range(per):
            q_buf[per * t + i, :, r] = res[:, i * DH:(i + 1) * DH].reshape(2, piece, DH)

    def dyn(chip):
        return (chip > c).astype(jnp.int32)

    near_static = [(0, 0, c), (1, 1, c), (1, 0, c), (1, 0, left_chip), (1, 0, right_chip)]
    near_dyn = [(dyn(left_chip), dyn(left_chip), left_chip), (dyn(right_chip), dyn(right_chip), right_chip)]
    far_blocks = [(1, 0, far_chip), (dyn(far_chip), dyn(far_chip), far_chip)]
    blocks = near_static + near_dyn + far_blocks

    def first_row(half, dev):
        return jnp.where(half == 0, dev, 2 * n - 1 - dev) * piece

    def make_bias():
        for b, (qs, ks, kc) in enumerate(blocks):
            for r in range(2):
                dev = 2 * c + r
                sq = seg_all[dev, pl.ds(qs, 1)]
                pq = first_row(qs, dev) + lax.broadcasted_iota(jnp.int32, (piece, piece), 1)
                for kr in range(2):
                    kd = 2 * kc + kr
                    sk = jnp.broadcast_to(seg_all[kd, pl.ds(ks, 1)], (piece, piece)).T
                    pk = first_row(ks, kd) + lax.broadcasted_iota(jnp.int32, (piece, piece), 0)
                    ok = (sq == sk) & (pk <= pq)
                    bias[b, pl.ds(kr * piece, piece), pl.ds(r * piece, piece)] = jnp.where(ok, 0.0, NEG).astype(F32)

    def scores(g, j, b):
        qs, ks, kc = blocks[b]
        q = q_buf[g * groups + j, qs].reshape(rows, DH)
        k = kv[g, ks, kc, :, 0].reshape(rows, DH)
        s = lax.dot_general(k, q, (((1,), (1,)), ((), ())), preferred_element_type=F32)
        return s + bias[b]

    def top(s):
        return jnp.max(s, axis=0, keepdims=True)

    def values(g, b):
        return jnp.concatenate([kv[g, blocks[b][1], blocks[b][2], r, 1] for r in range(2)], axis=1)

    def region(fn):
        pl.when(me >= 0)(fn)

    def attend(g, bs, first, last):
        def score_all():
            for j in range(groups):
                k = g * groups + j
                m = [None, None] if first else [m_buf[k, 0], m_buf[k, 1]]
                for i, b in enumerate(bs):
                    s = scores(g, j, b)
                    s_buf[j, i] = s
                    t = top(s)
                    half = blocks[b][0]
                    for f in range(2):
                        if isinstance(half, int):
                            v = t if half == f else None
                        else:
                            v = jnp.where(half == f, t, NEG)
                        if v is not None:
                            m[f] = v if m[f] is None else jnp.maximum(m[f], v)
                for f in range(2):
                    if not first:
                        c_buf[j, f] = jnp.exp2(m_buf[k, f] * SCALE - m[f] * SCALE)
                    m_buf[k, f] = m[f]

        def weigh_all():
            for j in range(groups):
                k = g * groups + j
                l, a = [0.0, 0.0], [0.0, 0.0]
                if not first:
                    l = [l_buf[k, f] * c_buf[j, f] for f in range(2)]
                    a = [a_buf[k, f] * c_buf[j, f] for f in range(2)]
                late = []
                for i, b in enumerate(bs):
                    half = blocks[b][0]
                    p = jnp.exp2(s_buf[j, i] * SCALE - m_buf[k, half] * SCALE)
                    lb = jnp.sum(p, axis=0, keepdims=True)
                    ab = jnp.dot(values(g, b), p.astype(BF16), preferred_element_type=F32)
                    if isinstance(half, int):
                        l[half], a[half] = l[half] + lb, a[half] + ab
                    else:
                        late.append((half, lb, ab))
                if last:
                    for f in range(2):
                        for half, lb, ab in late:
                            l[f] = l[f] + jnp.where(half == f, lb, 0.0)
                            a[f] = a[f] + jnp.where(half == f, ab, 0.0)
                        o = a[f] * (1.0 / l[f])
                        o_buf[g, f, :, :, pl.ds(j * DH, DH)] = o.T.astype(BF16).reshape(2, piece, DH)
                else:
                    for f in range(2):
                        l_buf[k, f], a_buf[k, f] = l[f], a[f]
                    for half, lb, ab in late:
                        l_buf[k, half] = l_buf[k, half] + lb
                        a_buf[k, half] = a_buf[k, half] + ab

        region(score_all)
        region(weigh_all)

    def here(g):
        attend(g, [0, 1, 2], True, False)

    def near(g):
        attend(g, [3, 4, 5, 6], False, False)

    def far(g):
        attend(g, [7, 8], False, True)

    def o_send(g):
        return remote(o_buf.at[g, :, other], o_sib.at[g], os_send, os_recv.at[g], sibling)

    nt = 3
    tile = wo.shape[-1] // nt

    def mine(g):
        return o_buf[g, :, h].reshape(rows, gw)

    def theirs(g):
        return o_sib[g].reshape(rows, gw)

    def project(lhs, rhs, first, last):
        for t in range(nt):
            col = pl.ds(t * tile, tile)
            acc = jnp.dot(lhs, rhs(col), preferred_element_type=F32)
            if not first:
                acc = acc + y_acc[:, col]
            if last:
                y_out[:, col] = acc.astype(BF16)
            else:
                y_acc[:, col] = acc

    def wo_wait(g):
        pltpu.make_async_copy(wo.at[g], wo.at[g], wo_sem.at[g]).wait()

    def out_proj(gs):
        lhs = []
        for g in gs:
            wo_wait(g)
            o_send(g).wait_recv()
            lhs += [mine(g), theirs(g)]
        project(jnp.concatenate(lhs, axis=-1),
                lambda col: wo[pl.ds(gs[0], len(gs)), :, col].reshape(len(gs) * 2 * gw, tile), gs[0] == 0, False)

    x_own = pltpu.make_async_copy(x_hbm, x_buf.at[:, h], x_sem)
    x_own.start()
    seg_own = pltpu.make_async_copy(seg_hbm, seg_all.at[me], seg_sem)
    seg_own.start()
    barrier = pltpu.get_barrier_semaphore()
    for d in range(1, n):
        pl.semaphore_signal(barrier, inc=1, device_id={"cp": lax.rem(me + d, n)}, device_id_type=pl.DeviceIdType.MESH)
    for g in range(heads):
        wkv_start(g)
    for t in range(n_q):
        wq_copy(t).start(priority=1)

    with ph("wait_x"):
        x_own.wait()
        seg_own.wait()

    with ph("barrier"):
        pl.semaphore_wait(barrier, n - 1)
    x_send = remote(x_buf.at[:, h], x_buf.at[:, h], xs_send, xs_recv, sibling)
    x_send.start()
    with ph("kv0a"):
        proj_head(0, h)
    send_rows(0, h)
    for d in range(1, n):
        remote(seg_all.at[me], seg_all.at[me], sg_send, sg_recv, lax.rem(me + d, n)).start()
    for g in range(heads):
        for cp in wo_copies(g):
            cp.start(priority=1)
    with ph("kv0c"):
        proj_head(1, h)
    send_rows(1, h)
    with ph("kv1a"):
        for g in range(2, heads):
            for part in range(parts):
                wkv_wait(g, part)
        proj_kv(1, h)
    with ph("qa"):
        for t in range(n_q - 1):
            wq_copy(t).wait()
            proj_q(t, h)
    with ph("wait_xs"):
        remote(x_buf.at[:, other], x_buf.at[:, other], xs_send, xs_recv, sibling).wait_recv()
    with ph("kv0b"):
        proj_kv(0, other)
    send_rows(0, other)
    send_rows(1, other)
    with ph("kv1b"):
        proj_kv(1, other)
    with ph("qb"):
        wq_copy(n_q - 1).wait()
        proj_q(n_q - 1, h)
        for t in range(n_q):
            proj_q(t, other)
    with ph("wait_seg"):
        remote(seg_others, seg_others, sg_send, sg_recv, sibling).wait_recv()
    with ph("bias"):
        make_bias()

    def near_rest(g):
        near_wait(g, 1, True)
        near_wait(g, 0, False)

    with ph("fwd0"):
        forward(0)
    send_first(2)
    send_second(2)
    with ph("here0"):
        here(0)
    with ph("nwait0"):
        near_rest(0)
    with ph("near0"):
        near(0)
    with ph("fwd1"):
        forward(1)
    send_first(3)
    with ph("here1"):
        here(1)
    with ph("nwait1"):
        near_rest(1)
    with ph("near1"):
        near(1)
    with ph("fwait0"):
        far_wait(0)
    with ph("far0"):
        far(0)
    o_send(0).start()
    with ph("here2"):
        here(2)
    with ph("fwd2"):
        forward(2)
    send_second(3)
    with ph("here3"):
        here(3)
    with ph("nwait2"):
        near_rest(2)
    with ph("near2"):
        near(2)
    with ph("fwait1"):
        far_wait(1)
    with ph("far1"):
        far(1)
    o_send(1).start()
    with ph("out0"):
        out_proj((0,))
    with ph("fwd3"):
        forward(3)
    with ph("out1"):
        out_proj((1,))
    with ph("fwait2"):
        far_wait(2)
    with ph("far2"):
        far(2)
    o_send(2).start()
    with ph("out2"):
        pl.when(h == 0)(lambda: out_proj((2,)))
    with ph("nwait3"):
        near_rest(3)
    with ph("near3"):
        near(3)
    with ph("out2b"):
        pl.when(h == 1)(lambda: out_proj((2,)))
    with ph("fwait3"):
        far_wait(3)
    with ph("far3"):
        attend(3, [7], False, False)
    with ph("fwait3b"):
        far_wait(3, 1)
    with ph("far3b"):
        attend(3, [8], False, True)
    o_send(3).start()
    wo_wait(3)
    with ph("out3a"):
        project(mine(3), lambda col: wo[3, pl.ds(0, gw), col], False, False)
    with ph("owait"):
        o_send(3).wait_recv()
    with ph("out3b"):
        project(theirs(3), lambda col: wo[3, pl.ds(gw, gw), col], False, True)

    with ph("drain"):
        x_send.wait_send()
        remote(seg_others, seg_others, sg_send, sg_recv, sibling).wait_send()
        for g in range(heads):
            sent = kv.at[g, :, pl.ds(0, chips - 1)]
            remote(sent, sent, kv_send.at[g], near_recv.at[0, 0, 0], right).wait_send()
        remote(o_sib, o_sib, os_send, os_recv.at[0], sibling).wait_send()


def solution(mesh):
    n = mesh.shape["cp"]
    chips = n // 2

    def local(x, seg, wq, wk, wv, wo):
        lq, d = x.shape
        piece = lq // 2
        kvh = wk.shape[1] // DH
        groups = wq.shape[1] // wk.shape[1]
        heads = kvh // 2
        qh = heads * groups
        dma = pltpu.SemaphoreType.DMA
        return pl.pallas_call(
            functools.partial(kernel, n, heads, groups),
            out_shape=pltpu.VMEM((lq, wo.shape[1]), BF16),
            in_specs=[pl.BlockSpec(memory_space=pl.ANY)] * 6,
            out_specs=pl.BlockSpec(memory_space=pltpu.VMEM),
            scratch_shapes=[
                pltpu.VMEM((2, 2, piece, d), BF16),
                pltpu.VMEM((heads // 2, d, 4 * DH), BF16),
                pltpu.VMEM((qh // 4, d, 4 * DH), BF16),
                pltpu.VMEM((heads, 2 * groups * DH, wo.shape[1]), BF16),
                pltpu.VMEM((heads, 2, chips, 2, 2, piece, DH), BF16),
                pltpu.VMEM((qh, 2, 2, piece, DH), BF16),
                pltpu.VMEM((n, 2, piece), jnp.int32),
                pltpu.VMEM((9, lq, lq), F32),
                pltpu.VMEM((groups, 4, lq, lq), F32),
                pltpu.VMEM((qh, 2, 1, lq), F32),
                pltpu.VMEM((qh, 2, 1, lq), F32),
                pltpu.VMEM((groups, 2, 1, lq), F32),
                pltpu.VMEM((qh, 2, DH, lq), F32),
                pltpu.VMEM((heads, 2, 2, piece, groups * DH), BF16),
                pltpu.VMEM((heads, 2, piece, groups * DH), BF16),
                pltpu.VMEM((lq, wo.shape[1]), F32),
                dma, dma, dma, dma, dma, dma,
                dma((heads, 4)), dma((qh // 4,)), dma((heads,)),
                dma((heads,)), dma((2, heads, 2)), dma((2, heads + 1)),
                dma, dma((heads,)),
            ],
            compiler_params=pltpu.CompilerParams(
                collective_id=0, has_side_effects=True, vmem_limit_bytes=67043328 - (2 << 20)),
            name="fused_attention",
        )(x.reshape(2, piece, d), seg.reshape(2, piece), wq, wk, wv, wo)

    rows = P(("dp", "cp"), None)
    return jax.shard_map(local, mesh=mesh, in_specs=(rows, P(("dp", "cp")), P(), P(), P(), P()), out_specs=rows, check_vma=False)
```

```python
import functools
import math

import jax
import jax.numpy as jnp
from jax import lax
from jax.experimental import pallas as pl
from jax.experimental.pallas import tpu as pltpu
from jax.sharding import PartitionSpec as P

DH = 128
F32 = jnp.float32
BF16 = jnp.bfloat16
NEG = float("-inf")
SCALE = math.log2(math.e) * DH ** -0.5


def kernel(
    n, heads, groups,
    x_hbm, seg_hbm, wq_hbm, wk_hbm, wv_hbm, wo_hbm, y_out,
    x_buf, wkv, wq, wo, kv, q_buf, seg_all, bias, s_buf, m_buf, l_buf, c_buf, a_buf, o_buf, o_sib, y_acc,
    x_sem, xs_send, xs_recv, seg_sem, sg_send, sg_recv, wkv_sem, wq_sem, wo_sem,
    kv_send, near_recv, far_recv, os_send, os_recv,
):
    chips = n // 2
    parts = wkv_sem.shape[1]
    piece = x_hbm.shape[1]
    rows = 2 * piece
    dim = x_hbm.shape[2]
    me = lax.axis_index("cp")
    c, h = lax.div(me, 2), lax.rem(me, 2)
    other = 1 - h
    right_chip, left_chip = lax.rem(c + 1, chips), lax.rem(c + chips - 1, chips)
    far_chip = lax.rem(c + chips // 2, chips)
    right, left, sibling = 2 * right_chip + h, 2 * left_chip + h, 2 * c + other
    qcols = heads * groups * DH
    gw = groups * DH
    ph = jax.named_scope

    def remote(src, dst, send, recv, dev):
        return pltpu.make_async_remote_copy(
            src_ref=src, dst_ref=dst, send_sem=send, recv_sem=recv,
            device_id={"cp": dev}, device_id_type=pl.DeviceIdType.MESH)

    def wkv_part(g, part):
        return (pl.ds(part * dim // parts, dim // parts), pl.ds(g % 2 * 2 * DH, 2 * DH))

    def wkv_at(g, part):
        return wkv_sem.at[g, part] if g < 2 else wkv_sem.at[2, 0]

    def wkv_start(g):
        col = pl.multiple_of((h * heads + g) * DH, DH)
        for part in range(parts):
            rng, at = wkv_part(g, part)
            for j, w in enumerate((wk_hbm, wv_hbm)):
                dst = wkv.at[g // 2, rng, pl.ds(at.start + j * DH, DH)]
                pltpu.make_async_copy(w.at[rng, pl.ds(col, DH)], dst, wkv_at(g, part)).start()

    def wkv_wait(g, part):
        ref = wkv.at[g // 2, *wkv_part(g, part)]
        pltpu.make_async_copy(ref, ref, wkv_at(g, part)).wait()

    qt = wq.shape[-1]
    n_q = wq.shape[0]

    def wq_copy(t):
        col = pl.multiple_of(h * qcols + t * qt, qt)
        return pltpu.make_async_copy(wq_hbm.at[:, pl.ds(col, qt)], wq.at[t], wq_sem.at[t])

    def wo_copies(g):
        res = []
        for i, core in enumerate((h, other)):
            row = pl.multiple_of(core * qcols + g * gw, DH)
            res.append(pltpu.make_async_copy(wo_hbm.at[pl.ds(row, gw)], wo.at[g, pl.ds(i * gw, gw)], wo_sem.at[g]))
        return res

    seg_others = seg_all.at[pl.ds(0, n - 1)]

    def own(g, r, to_right):
        s = 0 if to_right else 1
        ref = kv.at[g, :, c, r]
        return remote(ref, ref, kv_send.at[g], near_recv.at[s, g, r], right if to_right else left)

    def near_wait(g, r, from_left):
        s = 0 if from_left else 1
        ref = kv.at[g, :, left_chip if from_left else right_chip, r]
        remote(ref, ref, kv_send.at[g], near_recv.at[s, g, r], right if from_left else left).wait_recv()

    def halves(g):
        return ((g, slice(None)),) if g < heads - 1 else ((g, pl.ds(0, 1)), (heads, pl.ds(1, 1)))

    def fwd(g, to_right):
        s = 0 if to_right else 1
        refs = [(i, kv.at[g, f, left_chip if to_right else right_chip, s]) for i, f in halves(g)]
        return [remote(ref, ref, kv_send.at[g], far_recv.at[s, i], right if to_right else left) for i, ref in refs]

    def far_wait(g, half=0):
        i, f = halves(g)[half]
        for s in range(2):
            ref = kv.at[g, f, far_chip, s]
            remote(ref, ref, kv_send.at[g], far_recv.at[s, i], right if s == 0 else left).wait_recv()

    def forward(g):
        for to_right in (True, False):
            near_wait(g, 0 if to_right else 1, to_right)
            for cp in fwd(g, to_right):
                cp.start()

    def send_rows(g, r):
        own(g, r, True).start()
        own(g, r, False).start()

    def send_first(g):
        own(g, 0, True).start()
        own(g, 1, False).start()

    def send_second(g):
        own(g, 1, True).start()
        own(g, 0, False).start()

    def keep_kv(g, r, k, v):
        kv[g, :, c, r, 0] = k.astype(BF16).reshape(2, piece, DH)
        for f in range(2):
            kv[g, f, c, r, 1] = v[f * piece:(f + 1) * piece].T.astype(BF16)

    def proj_head(g, r):
        res = 0.0
        for part in range(parts):
            wkv_wait(g, part)
            rng, at = wkv_part(g, part)
            src = x_buf[:, r, :, rng].reshape(rows, rng.size)
            res = res + jnp.dot(src, wkv[g // 2, rng, at], preferred_element_type=F32)
        keep_kv(g, r, res[:, :DH], res[:, DH:])

    def proj_kv(t, r):
        src = x_buf[:, r].reshape(rows, dim)
        res = jnp.dot(src, wkv[t], preferred_element_type=F32)
        for i in range(2):
            k = 2 * i * DH
            keep_kv(2 * t + i, r, res[:, k:k + DH], res[:, k + DH:k + 2 * DH])

    def proj_q(t, r):
        src = x_buf[:, r].reshape(rows, dim)
        res = jnp.dot(src, wq[t], preferred_element_type=F32).astype(BF16)
        per = qt // DH
        for i in range(per):
            q_buf[per * t + i, :, r] = res[:, i * DH:(i + 1) * DH].reshape(2, piece, DH)

    def dyn(chip):
        return (chip > c).astype(jnp.int32)

    near_static = [(0, 0, c), (1, 1, c), (1, 0, c), (1, 0, left_chip), (1, 0, right_chip)]
    near_dyn = [(dyn(left_chip), dyn(left_chip), left_chip), (dyn(right_chip), dyn(right_chip), right_chip)]
    far_blocks = [(1, 0, far_chip), (dyn(far_chip), dyn(far_chip), far_chip)]
    blocks = near_static + near_dyn + far_blocks

    def first_row(half, dev):
        return jnp.where(half == 0, dev, 2 * n - 1 - dev) * piece

    def make_bias():
        for b, (qs, ks, kc) in enumerate(blocks):
            for r in range(2):
                dev = 2 * c + r
                sq = seg_all[dev, pl.ds(qs, 1)]
                pq = first_row(qs, dev) + lax.broadcasted_iota(jnp.int32, (piece, piece), 1)
                for kr in range(2):
                    kd = 2 * kc + kr
                    sk = jnp.broadcast_to(seg_all[kd, pl.ds(ks, 1)], (piece, piece)).T
                    pk = first_row(ks, kd) + lax.broadcasted_iota(jnp.int32, (piece, piece), 0)
                    ok = (sq == sk) & (pk <= pq)
                    bias[b, pl.ds(kr * piece, piece), pl.ds(r * piece, piece)] = jnp.where(ok, 0.0, NEG).astype(F32)

    def scores(g, j, b):
        qs, ks, kc = blocks[b]
        q = q_buf[g * groups + j, qs].reshape(rows, DH)
        k = kv[g, ks, kc, :, 0].reshape(rows, DH)
        s = lax.dot_general(k, q, (((1,), (1,)), ((), ())), preferred_element_type=F32)
        return s + bias[b]

    def top(s):
        return jnp.max(s, axis=0, keepdims=True)

    def values(g, b):
        return jnp.concatenate([kv[g, blocks[b][1], blocks[b][2], r, 1] for r in range(2)], axis=1)

    def region(fn):
        pl.when(me >= 0)(fn)

    def attend(g, bs, first, last):
        def score_all():
            for j in range(groups):
                k = g * groups + j
                m = [None, None] if first else [m_buf[k, 0], m_buf[k, 1]]
                for i, b in enumerate(bs):
                    s = scores(g, j, b)
                    s_buf[j, i] = s
                    t = top(s)
                    half = blocks[b][0]
                    for f in range(2):
                        if isinstance(half, int):
                            v = t if half == f else None
                        else:
                            v = jnp.where(half == f, t, NEG)
                        if v is not None:
                            m[f] = v if m[f] is None else jnp.maximum(m[f], v)
                for f in range(2):
                    if not first:
                        c_buf[j, f] = jnp.exp2(m_buf[k, f] * SCALE - m[f] * SCALE)
                    m_buf[k, f] = m[f]

        def weigh_all():
            for j in range(groups):
                k = g * groups + j
                l, a = [0.0, 0.0], [0.0, 0.0]
                if not first:
                    l = [l_buf[k, f] * c_buf[j, f] for f in range(2)]
                    a = [a_buf[k, f] * c_buf[j, f] for f in range(2)]
                late = []
                for i, b in enumerate(bs):
                    half = blocks[b][0]
                    p = jnp.exp2(s_buf[j, i] * SCALE - m_buf[k, half] * SCALE)
                    lb = jnp.sum(p, axis=0, keepdims=True)
                    ab = jnp.dot(values(g, b), p.astype(BF16), preferred_element_type=F32)
                    if isinstance(half, int):
                        l[half], a[half] = l[half] + lb, a[half] + ab
                    else:
                        late.append((half, lb, ab))
                if last:
                    for f in range(2):
                        for half, lb, ab in late:
                            l[f] = l[f] + jnp.where(half == f, lb, 0.0)
                            a[f] = a[f] + jnp.where(half == f, ab, 0.0)
                        o = a[f] * (1.0 / l[f])
                        o_buf[g, f, :, :, pl.ds(j * DH, DH)] = o.T.astype(BF16).reshape(2, piece, DH)
                else:
                    for f in range(2):
                        l_buf[k, f], a_buf[k, f] = l[f], a[f]
                    for half, lb, ab in late:
                        l_buf[k, half] = l_buf[k, half] + lb
                        a_buf[k, half] = a_buf[k, half] + ab

        region(score_all)
        region(weigh_all)

    def here(g):
        attend(g, [0, 1, 2], True, False)

    def near(g):
        attend(g, [3, 4, 5, 6], False, False)

    def far(g):
        attend(g, [7, 8], False, True)

    def o_send(g):
        return remote(o_buf.at[g, :, other], o_sib.at[g], os_send, os_recv.at[g], sibling)

    def o_start(g):
        for f in range(2):
            remote(o_buf.at[g, f, other], o_sib.at[g, f], os_send, os_recv.at[g], sibling).start()

    nt = 3
    tile = wo.shape[-1] // nt

    def mine(g):
        return o_buf[g, :, h].reshape(rows, gw)

    def theirs(g):
        return o_sib[g].reshape(rows, gw)

    def project(lhs, rhs, first, last):
        for t in range(nt):
            col = pl.ds(t * tile, tile)
            acc = jnp.dot(lhs, rhs(col), preferred_element_type=F32)
            if not first:
                acc = acc + y_acc[:, col]
            if last:
                y_out[:, col] = acc.astype(BF16)
            else:
                y_acc[:, col] = acc

    def wo_wait(g):
        pltpu.make_async_copy(wo.at[g], wo.at[g], wo_sem.at[g]).wait()

    def out_proj(gs):
        lhs = []
        for g in gs:
            wo_wait(g)
            o_send(g).wait_recv()
            lhs += [mine(g), theirs(g)]
        project(jnp.concatenate(lhs, axis=-1),
                lambda col: wo[pl.ds(gs[0], len(gs)), :, col].reshape(len(gs) * 2 * gw, tile), gs[0] == 0, False)

    x_own = pltpu.make_async_copy(x_hbm, x_buf.at[:, h], x_sem)
    x_own.start()
    seg_own = pltpu.make_async_copy(seg_hbm, seg_all.at[me], seg_sem)
    seg_own.start()
    barrier = pltpu.get_barrier_semaphore()
    for d in range(1, n):
        pl.semaphore_signal(barrier, inc=1, device_id={"cp": lax.rem(me + d, n)}, device_id_type=pl.DeviceIdType.MESH)
    for g in range(heads):
        wkv_start(g)
    for t in range(n_q):
        wq_copy(t).start(priority=1)

    with ph("wait_x"):
        x_own.wait()
        seg_own.wait()

    with ph("barrier"):
        pl.semaphore_wait(barrier, n - 1)
    x_send = remote(x_buf.at[:, h], x_buf.at[:, h], xs_send, xs_recv, sibling)
    x_send.start()
    with ph("kv0a"):
        proj_head(0, h)
    send_rows(0, h)
    for d in range(1, n):
        remote(seg_all.at[me], seg_all.at[me], sg_send, sg_recv, lax.rem(me + d, n)).start()
    for g in range(heads):
        for cp in wo_copies(g):
            cp.start(priority=1)
    with ph("kv0c"):
        proj_head(1, h)
    send_rows(1, h)
    with ph("kv1a"):
        pltpu.make_async_copy(wkv.at[1], wkv.at[1], wkv_at(2, 0)).wait()
        proj_kv(1, h)
    with ph("qa"):
        for t in range(n_q - 1):
            wq_copy(t).wait()
            proj_q(t, h)
    with ph("wait_xs"):
        remote(x_buf.at[:, other], x_buf.at[:, other], xs_send, xs_recv, sibling).wait_recv()
    with ph("kv0b"):
        proj_kv(0, other)
    send_rows(0, other)
    send_rows(1, other)
    with ph("kv1b"):
        proj_kv(1, other)
    with ph("qb"):
        wq_copy(n_q - 1).wait()
        proj_q(n_q - 1, h)
        for t in range(n_q):
            proj_q(t, other)
    with ph("wait_seg"):
        remote(seg_others, seg_others, sg_send, sg_recv, sibling).wait_recv()
    with ph("bias"):
        make_bias()

    def near_rest(g):
        near_wait(g, 1, True)
        near_wait(g, 0, False)

    with ph("fwd0"):
        forward(0)
    send_first(2)
    send_second(2)
    with ph("here0"):
        here(0)
    with ph("nwait0"):
        near_rest(0)
    with ph("near0"):
        near(0)
    with ph("fwd1"):
        forward(1)
    send_first(3)
    with ph("here1"):
        here(1)
    with ph("nwait1"):
        near_rest(1)
    with ph("near1"):
        near(1)
    with ph("fwait0"):
        far_wait(0)
    with ph("far0"):
        far(0)
    o_start(0)
    with ph("here2"):
        here(2)
    with ph("fwd2"):
        forward(2)
    send_second(3)
    with ph("here3"):
        here(3)
    with ph("nwait2"):
        near_rest(2)
    with ph("near2"):
        near(2)
    with ph("fwait1"):
        far_wait(1)
    with ph("far1"):
        far(1)
    o_start(1)
    with ph("out0"):
        out_proj((0,))
    with ph("fwd3"):
        forward(3)
    with ph("out1"):
        out_proj((1,))
    with ph("fwait2"):
        far_wait(2)
    with ph("far2"):
        far(2)
    o_start(2)
    with ph("out2"):
        pl.when(h == 0)(lambda: out_proj((2,)))
    with ph("nwait3"):
        near_rest(3)
    with ph("near3"):
        near(3)
    with ph("out2b"):
        pl.when(h == 1)(lambda: out_proj((2,)))
    with ph("fwait3"):
        far_wait(3)
    with ph("far3"):
        attend(3, [7], False, False)
    with ph("fwait3b"):
        far_wait(3, 1)
    with ph("far3b"):
        attend(3, [8], False, True)
    o_start(3)
    wo_wait(3)
    with ph("out3a"):
        project(mine(3), lambda col: wo[3, pl.ds(0, gw), col], False, False)
    with ph("owait"):
        o_send(3).wait_recv()
    with ph("out3b"):
        project(theirs(3), lambda col: wo[3, pl.ds(gw, gw), col], False, True)

    with ph("drain"):
        x_send.wait_send()
        remote(seg_others, seg_others, sg_send, sg_recv, sibling).wait_send()
        for g in range(heads):
            sent = kv.at[g, :, pl.ds(0, chips - 1)]
            remote(sent, sent, kv_send.at[g], near_recv.at[0, 0, 0], right).wait_send()
        remote(o_sib, o_sib, os_send, os_recv.at[0], sibling).wait_send()


def solution(mesh):
    n = mesh.shape["cp"]
    chips = n // 2

    def local(x, seg, wq, wk, wv, wo):
        lq, d = x.shape
        piece = lq // 2
        kvh = wk.shape[1] // DH
        groups = wq.shape[1] // wk.shape[1]
        heads = kvh // 2
        qh = heads * groups
        dma = pltpu.SemaphoreType.DMA
        return pl.pallas_call(
            functools.partial(kernel, n, heads, groups),
            out_shape=pltpu.VMEM((lq, wo.shape[1]), BF16),
            in_specs=[pl.BlockSpec(memory_space=pl.ANY)] * 6,
            out_specs=pl.BlockSpec(memory_space=pltpu.VMEM),
            scratch_shapes=[
                pltpu.VMEM((2, 2, piece, d), BF16),
                pltpu.VMEM((heads // 2, d, 4 * DH), BF16),
                pltpu.VMEM((qh // 4, d, 4 * DH), BF16),
                pltpu.VMEM((heads, 2 * groups * DH, wo.shape[1]), BF16),
                pltpu.VMEM((heads, 2, chips, 2, 2, piece, DH), BF16),
                pltpu.VMEM((qh, 2, 2, piece, DH), BF16),
                pltpu.VMEM((n, 2, piece), jnp.int32),
                pltpu.VMEM((9, lq, lq), F32),
                pltpu.VMEM((groups, 4, lq, lq), F32),
                pltpu.VMEM((qh, 2, 1, lq), F32),
                pltpu.VMEM((qh, 2, 1, lq), F32),
                pltpu.VMEM((groups, 2, 1, lq), F32),
                pltpu.VMEM((qh, 2, DH, lq), F32),
                pltpu.VMEM((heads, 2, 2, piece, groups * DH), BF16),
                pltpu.VMEM((heads, 2, piece, groups * DH), BF16),
                pltpu.VMEM((lq, wo.shape[1]), F32),
                dma, dma, dma, dma, dma, dma,
                dma((3, 4)), dma((qh // 4,)), dma((heads,)),
                dma((heads,)), dma((2, heads, 2)), dma((2, heads + 1)),
                dma, dma((heads,)),
            ],
            compiler_params=pltpu.CompilerParams(
                collective_id=0, has_side_effects=True, vmem_limit_bytes=67043328 - (2 << 20)),
            name="fused_attention",
        )(x.reshape(2, piece, d), seg.reshape(2, piece), wq, wk, wv, wo)

    rows = P(("dp", "cp"), None)
    return jax.shard_map(local, mesh=mesh, in_specs=(rows, P(("dp", "cp")), P(), P(), P(), P()), out_specs=rows, check_vma=False)
```
